32 devices in a mesh: ens: 2 (over y), gx: 4 (over z), col: 2 (over x), gz: 2 (over core).
Axes of the slice: x: 2, y: 2, z: 4, core: 2. Of those that a mesh axis runs over, the one named last changes fastest.
Arguments:
- checkpoints: bfloat16 [8, 3, 32, 8, 256], P(('ens', 'col'), None, 'gz', 'gx'), parts along dimension 0, may hold values from -3 to 3
- obs_values: float32 [8, 32, 8, 256], P('ens', 'gz', 'gx', 'col'), parts along dimension 0, may hold values from -3 to 3
- obs_mask: int32 [8, 32, 8, 256], P('ens', 'gz', 'gx', 'col'), parts along dimension 0, may hold values 0 or 1
- drag: float32 [64], P(('ens', 'gz')), parts along dimension 0, may hold values from 0.05 to 0.5
Outputs:
- grad_init: float32 [6, 32, 8, 256], P('ens', 'gz', 'gx', 'col'), parts along dimension 0
- cost_levels: float32 [64], P(('ens', 'gz')), parts along dimension 0
- drag_grad: float32 [64], P(('ens', 'gz')), parts along dimension 0
The draws below stay inside these ranges and needn't reach their ends.
There are 2 independent parts, one for each index of `ens`. The reference program is written for one: setup_inputs(seed, part) draws one part's arguments, and reference() takes and returns one part's arrays. A program takes and returns all parts, laid end to end along the dimension named above; each array names one. Nothing has to cross between parts.
All inputs are finite; a program needn't handle non-finite values. No bound on the sum of `obs_mask` on one device may be relied on, other than what follows from the above.
Results may differ from the reference program's by a relative error of at most 0.0003.
Values may be sent and summed in bfloat16 or wider, within the bound.
A program may use at most 64 MiB of HBM per device.

```python
import math
import jax
import jax.numpy as jnp
from jax import lax

NLEV = 32
NSEG = 4
SEG = 2
NX = 8
NY = 256


def set_ends(array, own_key, smallest, largest):
    spot = [jax.random.randint(jax.random.fold_in(own_key, axis), (), 0, length) for axis, length in enumerate(array.shape)]
    longest = array.shape.index(max(array.shape))
    next_to = spot[:longest] + [(spot[longest] + 1) % array.shape[longest]] + spot[longest + 1:]
    return array.at[tuple(spot)].set(smallest).at[tuple(next_to)].set(largest)


def level_of(rng, dims, pieces, least, high):
    def one(position, blocks):
        steps = jax.random.uniform(jax.random.fold_in(jax.random.fold_in(rng, 6), position), (blocks,), jnp.float32, least / len(pieces), high / len(pieces))
        return jnp.repeat(jnp.exp(steps), dims[position] // blocks).reshape((-1,) + (1,) * (len(dims) - position - 1))

    loudness = one(*pieces[0])
    for cut in pieces[1:]:
        loudness = loudness * one(*cut)
    return loudness


def bell_draw(rng, shape, spread, limit, split=(), dtype=jnp.bfloat16):
    result = jax.random.normal(rng, shape, jnp.float32) * spread
    if len(split) > 0:
        result = level_of(rng, shape, split, -0.22, 0.18) * result
    return jnp.clip(result, min=-limit, max=limit).astype(dtype)


def setup_inputs(seed: int = 0, part: int = 0) -> dict:
    seeds = jax.random.split(jax.random.key(seed), 5)
    part_splits = jax.random.split(jax.random.fold_in(seeds[4], part), 5)
    checkpoints = bell_draw(part_splits[0], (NSEG, 3, NLEV, NX, NY), 0.5, 3.0, ((0, 2), (2, 2), (3, 4)))
    obs_values = bell_draw(part_splits[1], (NSEG, NLEV, NX, NY), 0.5, 3.0, ((1, 2), (2, 4), (3, 2)), jnp.float32)
    obs_mask = set_ends((jax.random.randint(part_splits[2], (NSEG, NLEV, NX, NY), 0, 3) < 1).astype(jnp.int32), jax.random.fold_in(part_splits[2], 1), 0, 1)
    drag = jnp.clip(jnp.exp(math.log(0.5) - 2.3025851 * jax.random.uniform(part_splits[3], (NLEV,), jnp.float32) ** level_of(part_splits[3], (NLEV,), ((0, 2),), -0.2, 0.2)), 0.05, 0.5)
    return {"checkpoints": checkpoints, "obs_values": obs_values, "obs_mask": obs_mask, "drag": drag}


time_step = 0.1
viscosity = 0.05
vertical_mix = 0.2

def along_cols(a):
    return 0.5 * (a[:, 1:-1, 2:] - a[:, 1:-1, :-2])

def along_rows(a):
    return 0.5 * (a[:, 2:, 1:-1] - a[:, :-2, 1:-1])

def laplace(a):
    return a[:, 2:, 1:-1] + a[:, :-2, 1:-1] + a[:, 1:-1, 2:] + a[:, 1:-1, :-2] - 4.0 * a[:, 1:-1, 1:-1]

def advance(padded, drag, coriolis):
    levels = padded[:, 1:-1]
    thick, zonal, merid = (levels[0], levels[1], levels[2])
    centre = padded[:, 1:-1, 1:-1, 1:-1]
    h_c, u_c, v_c = (centre[0], centre[1], centre[2])
    rot = coriolis[None, :, None]
    rate = drag[:, None, None]
    vert = padded[:, 2:, 1:-1, 1:-1] + padded[:, :-2, 1:-1, 1:-1] - 2.0 * centre
    u_new = u_c + time_step * (-along_cols(thick) - u_c * along_cols(zonal) - v_c * along_rows(zonal) + rot * v_c - rate * u_c) + viscosity * laplace(zonal)
    v_new = v_c + time_step * (-along_rows(thick) - u_c * along_cols(merid) - v_c * along_rows(merid) - rot * u_c - rate * v_c) + viscosity * laplace(merid)
    h_new = h_c - time_step * (along_cols(zonal) + along_rows(merid) + along_cols(thick * zonal) + along_rows(thick * merid)) + viscosity * laplace(thick)
    return jnp.stack([h_new, u_new, v_new]) + vertical_mix * vert

def reference(checkpoints, obs_values, obs_mask, drag):
    rows = jnp.arange(NX).astype(jnp.float32)
    cols = jnp.arange(NY).astype(jnp.float32)
    coriolis = 0.2 + 0.1 * rows / NX
    weight = (1.0 + 2.0 * rows / NX)[:, None] * (1.0 + 2.0 * cols / NY)[None, :]
    adjoint = jnp.zeros((3, NLEV, NX, NY), jnp.float32)
    cost = jnp.zeros((NLEV,), jnp.float32)
    drag_total = jnp.zeros((NLEV,), jnp.float32)
    for seg in reversed(range(NSEG)):
        state = checkpoints[seg].astype(jnp.float32)
        pads = []
        for step in range(SEG):
            padded = jnp.pad(state, ((0, 0), (1, 1), (1, 1), (1, 1)))
            pads.append(padded)
            state = advance(padded, drag, coriolis)
        resid = state[0] - obs_values[seg]
        forcing = weight[None] * obs_mask[seg].astype(jnp.float32) * resid
        cost = cost + 0.5 * lax.optimization_barrier(jnp.sum(forcing * resid, axis=(1, 2)))
        adjoint = adjoint.at[0].add(forcing)
        for step in reversed(range(SEG)):

            def local(padded, rate):
                return advance(padded, rate, coriolis)
            unused, pull = jax.vjp(local, pads[step], drag)
            cot_pad, cot_drag = pull(adjoint)
            drag_total = drag_total + cot_drag
            adjoint = cot_pad[:, 1:-1, 1:-1, 1:-1]
    scale = 1.0 / (NX * NY)
    return (adjoint, cost * scale, drag_total * scale)
```

```python
import functools

import jax
import jax.numpy as jnp
from jax import lax
from jax.experimental import pallas as pl
from jax.experimental.pallas import tpu as pltpu
from jax.sharding import PartitionSpec as P

SEG = 2


time_step = 0.1
viscosity = 0.05
vertical_mix = 0.2


def with_halo(x, sides, width):
    for axis, dim in sides:
        devices, length = (lax.axis_size(axis), x.shape[dim])
        up = [(i, (i + 1) % devices) for i in range(devices - 1)]
        down = [(j, i) for i, j in up]
        last = lax.slice_in_dim(x, length - width, length, axis=dim)
        initial = lax.slice_in_dim(x, 0, width, axis=dim)
        before = lax.ppermute(last, axis, up)
        after = lax.ppermute(initial, axis, down)
        x = jnp.concatenate([before, x, after], axis=dim)
    return x


def passed_along(block, axis, distance):
    devices = range(lax.axis_size(axis))
    route = [(i - distance, i) for i in devices if i - distance in devices]
    return lax.ppermute(block, axis, route)


def along_cols(a):
    return 0.5 * (a[:, 1:-1, 2:] - a[:, 1:-1, :-2])


def along_rows(a):
    return 0.5 * (a[:, 2:, 1:-1] - a[:, :-2, 1:-1])


def laplace(a):
    return (
        a[:, 2:, 1:-1] + a[:, :-2, 1:-1] + a[:, 1:-1, 2:] + a[:, 1:-1, :-2] - 4.0 * a[:, 1:-1, 1:-1]
    )


def advance(padded, drag, coriolis):
    levels = padded[:, 1:-1]
    thick, zonal, merid = (levels[0], levels[1], levels[2])
    centre = padded[:, 1:-1, 1:-1, 1:-1]
    h_c, u_c, v_c = (centre[0], centre[1], centre[2])
    rot = coriolis[None, :, None]
    rate = drag[:, None, None]
    vert = padded[:, 2:, 1:-1, 1:-1] + padded[:, :-2, 1:-1, 1:-1] - 2.0 * centre
    u_new = (
        u_c
        + time_step
        * (
            -along_cols(thick)
            - u_c * along_cols(zonal)
            - v_c * along_rows(zonal)
            + rot * v_c
            - rate * u_c
        )
        + viscosity * laplace(zonal)
    )
    v_new = (
        v_c
        + time_step
        * (
            -along_rows(thick)
            - u_c * along_cols(merid)
            - v_c * along_rows(merid)
            - rot * u_c
            - rate * v_c
        )
        + viscosity * laplace(merid)
    )
    h_new = (
        h_c
        - time_step
        * (
            along_cols(zonal)
            + along_rows(merid)
            + along_cols(thick * zonal)
            + along_rows(thick * merid)
        )
        + viscosity * laplace(thick)
    )
    return jnp.stack([h_new, u_new, v_new]) + vertical_mix * vert


def extend(state):
    return with_halo(state, (("gx", 2), ("col", 3), ("gz", 1)), 1)


def halo_back(cot):
    inner = cot[:, 1:-1, 1:-1, 1:-1]
    below = passed_along(cot[:, 0, 1:-1, 1:-1], "gz", -1)
    above = passed_along(cot[:, -1, 1:-1, 1:-1], "gz", 1)
    inner = inner.at[:, -1].add(below).at[:, 0].add(above)
    south = passed_along(cot[:, 1:-1, 0, 1:-1], "gx", -1)
    north = passed_along(cot[:, 1:-1, -1, 1:-1], "gx", 1)
    inner = inner.at[:, :, -1].add(south).at[:, :, 0].add(north)
    west = passed_along(cot[:, 1:-1, 1:-1, 0], "col", -1)
    east = passed_along(cot[:, 1:-1, 1:-1, -1], "col", 1)
    return inner.at[:, :, :, -1].add(west).at[:, :, :, 0].add(east)


def on_device(checkpoints, obs_values, obs_mask, drag):
    lat_count = obs_values.shape[2]
    lon_count = obs_values.shape[3]
    segments = obs_values.shape[0]
    total_lat = lat_count * lax.axis_size("gx")
    total_lon = lon_count * lax.axis_size("col")
    rows = (lax.axis_index("gx") * lat_count + jnp.arange(lat_count)).astype(jnp.float32)
    cols = (lax.axis_index("col") * lon_count + jnp.arange(lon_count)).astype(jnp.float32)
    coriolis = 0.2 + 0.1 * rows / total_lat
    weight = (1.0 + 2.0 * rows / total_lat)[:, None] * (1.0 + 2.0 * cols / total_lon)[None, :]
    owned_cols = lax.all_to_all(checkpoints, "col", split_axis=4, concat_axis=0, tiled=True)

    def local(padded, rate):
        return advance(padded, rate, coriolis)

    levels = drag.shape[0]
    adjoint = jnp.zeros((3, levels, lat_count, lon_count), jnp.float32)
    cost = jnp.zeros((levels,), jnp.float32)
    drag_total = jnp.zeros((levels,), jnp.float32)
    for seg in reversed(range(segments)):
        state = owned_cols[seg].astype(jnp.float32)
        pads = []
        for step in range(SEG):
            padded = extend(state)
            pads.append(padded)
            state = advance(padded, drag, coriolis)
        resid = state[0] - obs_values[seg]
        forcing = weight[None] * obs_mask[seg].astype(jnp.float32) * resid
        seg_cost = 0.5 * jnp.sum(forcing * resid, axis=(1, 2))
        adjoint = adjoint.at[0].add(forcing)
        seg_drag = jnp.zeros((levels,), jnp.float32)
        for step in reversed(range(SEG)):
            unused, pull = jax.vjp(local, pads[step], drag)
            cot_pad, cot_drag = pull(adjoint)
            seg_drag = seg_drag + cot_drag
            adjoint = halo_back(cot_pad)
        summed_drag, summed_cost = lax.psum((seg_drag, seg_cost), ("gx", "col"))
        drag_total = drag_total + summed_drag
        cost = cost + summed_cost
    scale = 1.0 / (total_lat * total_lon)
    return (adjoint, cost * scale, drag_total * scale)


MESH = pl.DeviceIdType.MESH
UNSEEN = 1e30
TILE = 8
PAD = 8


def sweep_kernel(
    zn, levels, lat, lon, ck, obs, mask, drag, out, cost, dgrad,
    stage, seam, ckg, omg, oms, dragb, xs, xt, lam, lamt, acc, fsend, frecv, xrecv,
    send, rck, rckr, rom, romr, rst, rstr, rdrag, rfin, rxfin,
):
    local_segs = ck.shape[0]
    segments = obs.shape[0]
    x, c, g = (lax.axis_index(a) for a in ("gx", "col", "gz"))
    oc, og = 1 - c, 1 - g
    half = levels * lat
    total = 2 * half
    block = total // zn
    strip = lon // zn
    reach = SEG * (segments + 1)
    inner = strip - reach
    last = segments - 1
    mine = pl.ds(pl.multiple_of(g * half, half), half)
    theirs = pl.ds(pl.multiple_of(og * half, half), half)
    base = x * block + g * TILE
    f32 = jnp.float32
    sent = []

    def copy_of(src, dst, sem, where, slot):
        return pltpu.make_async_remote_copy(
            src_ref=src, dst_ref=dst, send_sem=send.at[slot], recv_sem=sem,
            device_id=where, device_id_type=MESH,
        )

    def put(src, dst, sem, where, when=None, starts=None):
        copy = copy_of(src, dst, sem, where, len(sent))
        sent.append((copy, when))
        if starts is not None:
            starts.append((copy, when))
        elif when is None:
            copy.start()
        else:
            pl.when(when)(copy.start)

    def arrived(dst, sem, when=None):
        copy = copy_of(dst, dst, sem, {"gz": og}, 0)
        if when is None:
            copy.wait_recv()
        else:
            pl.when(when)(copy.wait_recv)

    def around(d):
        return lax.rem(x + d, zn)

    barrier = pltpu.get_barrier_semaphore()
    for dc in range(2):
        for dz in range(zn):
            for dg in range(2):
                if dc or dz or dg:
                    peer = {"gx": around(dz), "col": oc if dc else c, "gz": og if dg else g}
                    pl.semaphore_signal(barrier, inc=1, device_id=peer, device_id_type=MESH)

    for s in range(segments):
        omg[s, x, mine, :] = jnp.where(mask[s] != 0, obs[s], UNSEEN)

    lane = lax.broadcasted_iota(jnp.int32, (TILE, lon), 1)
    group, spot = lane // strip, lane % strip
    wide_lane = lax.broadcasted_iota(jnp.int32, (half, lon), 1)
    wide_group = wide_lane // strip
    shift_of = [inner, reach]
    for s in range(local_segs):
        whole = [ck[s, f].astype(f32) for f in range(3)]
        for to in range(2):
            packed = jnp.zeros((half, lon), f32)
            for f in range(3):
                stage[s, to, f] = ck[s, f, :, to * lon : (to + 1) * lon]
                near = jnp.where(wide_lane >= lon // 2, whole[f][:, :lon], whole[f][:, lon:])
                packed = jnp.where(
                    wide_group == f, pltpu.roll(near, (f * strip + shift_of[to]) % lon, 1), packed
                )
            stage[s, to, 3] = packed.astype(ck.dtype)
    for to in range(2):
        packed = jnp.zeros((half, lon), f32)
        for s in range(segments):
            masked = jnp.where(mask[s] != 0, obs[s], UNSEEN)
            packed = jnp.where(
                wide_group == s, pltpu.roll(masked, (s * strip + shift_of[to]) % lon, 1), packed
            )
        seam[to] = packed
    own = [c * local_segs + s for s in range(local_segs)]
    for s in range(local_segs):
        ckg[own[s], :, x, mine, :] = stage[s, c]
    oms[c, x, mine, :] = seam[c]

    col_lane = lax.broadcasted_iota(jnp.int32, (half, levels), 1)
    sub = lax.broadcasted_iota(jnp.int32, (half, levels), 0)
    spread = jnp.sum(
        jnp.where(sub // lat == col_lane, jnp.broadcast_to(drag[...], (half, levels)), 0.0),
        axis=1, keepdims=True,
    )
    dragb[mine, :] = jnp.broadcast_to(spread, (half, lon))
    pl.semaphore_wait(barrier, 4 * zn - 1)

    def rows_of(b):
        return pl.ds(pl.multiple_of(b * block, block), block)

    def near_by(b, j, a):
        return jnp.logical_and(b - j <= a, j - b <= a)

    blocks = half // block
    held = [g * blocks + i for i in range(blocks)]
    theirs_held = [og * blocks + i for i in range(blocks)]

    def reach_of(seg):
        return 2 if seg == last else 1

    def own_reach(s):
        return jnp.where(own[s] == last, 2, 1)

    def send_ck(s):
        starts = []
        for dz in (2, 1, 3, 0):
            for dc in (1, 0):
                if not (dc or dz):
                    continue
                j, to = around(dz), oc if dc else c
                for i in range(blocks):
                    put(
                        stage.at[s, to, :, i * block : (i + 1) * block, :],
                        ckg.at[own[s], :, x, rows_of(held[i]), :],
                        rck.at[own[s], x, i], {"gx": j, "col": to},
                        near_by(held[i], j, own_reach(s)), starts,
                    )
        return starts

    def send_om(seg):
        for dz in (2, 1, 3):
            j = around(dz)
            for i in range(blocks):
                part = omg.at[seg, x, rows_of(held[i]), :]
                put(part, part, rom.at[seg, x, i], {"gx": j}, near_by(held[i], j, 1))

    def send_seam():
        for dz in (2, 1, 3, 0):
            for dc in (1, 0):
                if not (dc or dz):
                    continue
                j, to = around(dz), oc if dc else c
                for i in range(blocks):
                    put(
                        seam.at[to, i * block : (i + 1) * block, :],
                        oms.at[c, x, rows_of(held[i]), :],
                        rst.at[c, x, i], {"gx": j, "col": to}, near_by(held[i], j, 1),
                    )

    def start(starts, also):
        for copy, when in starts:
            pl.when(jnp.logical_and(when, also))(copy.start)

    order = list(reversed(range(local_segs)))
    ck_starts = {s: send_ck(s) for s in order}
    ahead, behind = c == 1, c == 0
    start(ck_starts[order[0]], ahead)
    send_om(last)
    send_seam()
    put(dragb.at[mine], dragb.at[mine], rdrag, {"gz": og})
    start(ck_starts[order[1]], ahead)
    send_om(last - 1)
    start(ck_starts[order[0]], behind)
    send_om(last - 2)
    start(ck_starts[order[1]], behind)
    send_om(last - 3)

    xs[...] = jnp.zeros_like(xs)
    xt[...] = jnp.zeros_like(xt)
    lam[...] = jnp.zeros_like(lam)
    lamt[...] = jnp.zeros_like(lamt)
    acc[...] = jnp.zeros_like(acc)

    def pass_ck(seg):
        source = seg // local_segs
        for i in range(blocks):
            wanted = near_by(held[i], x, reach_of(seg))
            for z in range(zn):
                here = jnp.logical_and(c == source, x == z)
                arrived(
                    ckg.at[seg, :, z, rows_of(held[i]), :], rck.at[seg, z, i],
                    jnp.logical_and(wanted, jnp.logical_not(here)),
                )
            part = ckg.at[seg, :, :, rows_of(held[i]), :]
            put(part, part, rckr.at[seg, i], {"gz": og}, wanted)

    def pass_om(seg):
        for i in range(blocks):
            wanted = near_by(held[i], x, 1)
            for z in range(zn):
                arrived(
                    omg.at[seg, z, rows_of(held[i]), :], rom.at[seg, z, i],
                    jnp.logical_and(wanted, x != z),
                )
            part = omg.at[seg, :, rows_of(held[i]), :]
            put(part, part, romr.at[seg, i], {"gz": og}, wanted)

    def pass_seam():
        for i in range(blocks):
            wanted = near_by(held[i], x, 1)
            for source in range(2):
                for z in range(zn):
                    here = jnp.logical_and(c == source, x == z)
                    arrived(
                        oms.at[source, z, rows_of(held[i]), :], rst.at[source, z, i],
                        jnp.logical_and(wanted, jnp.logical_not(here)),
                    )
            part = oms.at[:, :, rows_of(held[i]), :]
            put(part, part, rstr.at[i], {"gz": og}, wanted)

    def take_ck(seg):
        for i in range(blocks):
            arrived(
                ckg.at[seg, :, :, rows_of(theirs_held[i]), :], rckr.at[seg, i],
                near_by(theirs_held[i], x, reach_of(seg)),
            )

    def take_om(seg):
        for i in range(blocks):
            arrived(
                omg.at[seg, :, rows_of(theirs_held[i]), :], romr.at[seg, i],
                near_by(theirs_held[i], x, 1),
            )

    def take_seam():
        for i in range(blocks):
            arrived(
                oms.at[:, :, rows_of(theirs_held[i]), :], rstr.at[i],
                near_by(theirs_held[i], x, 1),
            )

    at_row = lax.broadcasted_iota(jnp.int32, (TILE, lon), 0) % lat
    first_lane, last_lane = lane == 0, lane == lon - 1
    first_row, last_row = at_row == 0, at_row == lat - 1
    first_group, last_group = group == 0, group == zn - 1
    row_f = at_row.astype(f32)
    total_lat, total_lon = float(zn * lat), float(2 * lon)
    col = lane + c * lon
    seam_start = lon - jnp.where(c == 0, inner, reach)
    seam_col = spot + seam_start
    seam_row = row_f + (group * lat).astype(f32)
    half_step = 0.5 * time_step
    keep = 1.0 - 4.0 * viscosity - 2.0 * vertical_mix

    def turn_of(row):
        return time_step * (0.2 + 0.1 * row / total_lat)

    def weight_of(row, column):
        return (1.0 + 2.0 * row / total_lat) * (1.0 + 2.0 * column.astype(f32) / total_lon)

    turns = [turn_of(row_f + float(z * lat)) for z in range(zn)] + [turn_of(seam_row)]
    weights = [weight_of(row_f + float(z * lat), col) for z in range(zn)]
    weights.append(weight_of(seam_row, seam_col))

    class Main:
        def __init__(self, ref, lead, f, z, o):
            self.spot = (ref, lead, f, z, o)

        def at(self, dz, shift):
            ref, lead, f, z, o = self.spot
            return ref[lead, f, z + 1 + dz, pl.ds(o + shift, TILE), :]

        def centre(self):
            return self.at(0, 0)

        def east(self, a):
            return jnp.where(last_lane, 0.0, pltpu.roll(a, lon - 1, 1))

        def west(self, a):
            return jnp.where(first_lane, 0.0, pltpu.roll(a, 1, 1))

        def north(self):
            return jnp.where(last_row, self.at(1, 1 - lat), self.at(0, 1))

        def south(self):
            return jnp.where(first_row, self.at(-1, lat - 1), self.at(0, -1))

        def mixed(self):
            return self.at(0, lat) + self.at(0, -lat)

    class Seam(Main):
        def at(self, dz, shift):
            ref, lead, f, z, o = self.spot
            return ref[lead, f, pl.ds(o + shift, TILE), :]

        def east(self, a):
            return pltpu.roll(a, lon - 1, 1)

        def west(self, a):
            return pltpu.roll(a, 1, 1)

        def north(self):
            above = jnp.where(last_group, 0.0, pltpu.roll(self.at(0, 1 - lat), lon - strip, 1))
            return jnp.where(last_row, above, self.at(0, 1))

        def south(self):
            below = jnp.where(first_group, 0.0, pltpu.roll(self.at(0, lat - 1), strip, 1))
            return jnp.where(first_row, below, self.at(0, -1))

    def cells(kind, lead, z, o):
        view = Main if z < zn else Seam
        ref = ((xs, xt), (lam, lamt))[kind][z == zn]
        return [view(ref, lead, f, z, o) for f in range(3)]

    def keep_at(kind, lead, f, z, m, value):
        rows = pl.ds(m + PAD, TILE)
        if z < zn:
            (xs, lam)[kind][lead, f, z + 1, rows, :] = value
        else:
            (xt, lamt)[kind][lead, f, rows, :] = value

    def step(src, z, o, dt_drag):
        H, U, V = cells(0, src, z, o)
        h, u, v = H.centre(), U.centre(), V.centre()
        h_e, u_e, v_e = H.east(h), U.east(u), V.east(v)
        h_w, u_w, v_w = H.west(h), U.west(u), V.west(v)
        h_n, u_n, v_n = H.north(), U.north(), V.north()
        h_s, u_s, v_s = H.south(), U.south(), V.south()
        u_dx, u_dy = u_e - u_w, u_n - u_s
        v_dx, v_dy = v_e - v_w, v_n - v_s
        h_new = (
            keep * h
            + viscosity * ((h_n + h_s) + (h_e + h_w))
            - half_step * ((u_dx + v_dy) + (h_e * u_e - h_w * u_w) + (h_n * v_n - h_s * v_s))
            + vertical_mix * H.mixed()
        )
        u_new = (
            keep * u
            + viscosity * ((u_n + u_s) + (u_e + u_w))
            - half_step * ((h_e - h_w) + u * u_dx + v * u_dy)
            + (turns[z] * v - dt_drag * u)
            + vertical_mix * U.mixed()
        )
        v_new = (
            keep * v
            + viscosity * ((v_n + v_s) + (v_e + v_w))
            - half_step * ((h_n - h_s) + u * v_dx + v * v_dy)
            - (turns[z] * u + dt_drag * v)
            + vertical_mix * V.mixed()
        )
        return h_new, u_new, v_new

    def thickness(src, z, o):
        H, U, V = cells(0, src, z, o)
        h, u = H.centre(), U.centre()
        h_e, u_e, h_w, u_w = H.east(h), U.east(u), H.west(h), U.west(u)
        h_n, v_n = H.north(), V.north()
        h_s, v_s = H.south(), V.south()
        return (
            keep * h
            + viscosity * ((h_n + h_s) + (h_e + h_w))
            - half_step
            * ((u_e - u_w) + (v_n - v_s) + (h_e * u_e - h_w * u_w) + (h_n * v_n - h_s * v_s))
            + vertical_mix * H.mixed()
        )

    def adjoint(src, lead, z, o, dt_drag):
        H, U, V = cells(0, src, z, o)
        A, B, D = cells(1, lead, z, o)
        turn = turns[z]
        h, u, v = H.centre(), U.centre(), V.centre()
        a, b, d = A.centre(), B.centre(), D.centre()
        u_e, v_e, u_w, v_w = U.east(u), V.east(v), U.west(u), V.west(v)
        u_n, v_n, u_s, v_s = U.north(), V.north(), U.south(), V.south()
        a_e, b_e, d_e = A.east(a), B.east(b), D.east(d)
        a_w, b_w, d_w = A.west(a), B.west(b), D.west(d)
        a_n, b_n, d_n = A.north(), B.north(), D.north()
        a_s, b_s, d_s = A.south(), B.south(), D.south()
        a_dx, a_dy = a_e - a_w, a_n - a_s
        deep = 1.0 + h
        new_a = (
            keep * a
            + viscosity * ((a_n + a_s) + (a_e + a_w))
            + half_step * ((b_e - b_w) + (d_n - d_s) + u * a_dx + v * a_dy)
            + vertical_mix * A.mixed()
        )
        new_b = (
            keep * b
            + viscosity * ((b_n + b_s) + (b_e + b_w))
            + half_step
            * (
                (u_e * b_e - u_w * b_w)
                + (v_n * b_n - v_s * b_s)
                + deep * a_dx
                - (b * (u_e - u_w) + d * (v_e - v_w))
            )
            - (dt_drag * b + turn * d)
            + vertical_mix * B.mixed()
        )
        new_d = (
            keep * d
            + viscosity * ((d_n + d_s) + (d_e + d_w))
            + half_step
            * (
                (u_e * d_e - u_w * d_w)
                + (v_n * d_n - v_s * d_s)
                + deep * a_dy
                - (b * (u_n - u_s) + d * (v_n - v_s))
            )
            + (turn * b - dt_drag * d)
            + vertical_mix * D.mixed()
        )
        return (new_a, new_b, new_d), u * b + v * d

    def over(halo, work):
        count = min(total // TILE, 1 + -(-2 * halo * lat // TILE))
        begin = jnp.clip(base - halo * lat, 0, total - count * TILE)

        def body(i, carry):
            work(begin + i * TILE)
            return carry

        lax.fori_loop(0, count, body, 0)

    def unpack(seg):
        def body(b, carry):
            rows = rows_of(b)
            to = pl.ds(pl.multiple_of(b * block + PAD, TILE), block)
            for f in range(3):
                for z in range(zn):
                    xs[0, f, z + 1, to, :] = ckg[seg, f, z, rows, :].astype(f32)
            lanes = lax.broadcasted_iota(jnp.int32, (block, lon), 1) // strip
            parts = [ckg[seg, 3, z, rows, :].astype(f32) for z in range(zn)]
            for f in range(3):
                value = parts[0]
                for z in range(zn):
                    turned = parts[z]
                    if z != f:
                        turned = pltpu.roll(turned, ((z - f) * strip) % lon, 1)
                    value = jnp.where(lanes == z, turned, value) if z else turned
                xt[0, f, to, :] = value
            return carry

        a = reach_of(seg)
        low, high = jnp.maximum(x - a, 0), jnp.minimum(x + a, zn - 1)
        lax.fori_loop(low, high + 1, body, 0)

    far_seam = spot >= jnp.where(c == 0, inner, reach)

    now = 0
    pass_ck(last)
    pass_om(last)
    pass_seam()
    take_ck(last)
    arrived(dragb.at[theirs], rdrag)
    for seg in reversed(range(segments)):
        remaining = SEG * (seg + 1)
        if seg < last:
            pass_om(seg)
            take_ck(seg)
        unpack(seg)

        def first(m):
            dt_drag = dragb[pl.ds(m, TILE), :] * time_step
            for z in range(zn + 1):
                for f, value in enumerate(step(0, z, m + PAD, dt_drag)):
                    keep_at(0, 1, f, z, m, value)

        over(remaining + 1, first)
        take_om(seg)
        if seg == last:
            take_seam()

        def force(m):
            rows = pl.ds(m, TILE)
            merged = None
            for z in range(zn):
                near = jnp.where(far_seam, oms[1, z, rows, :], oms[0, z, rows, :])
                if z != seg:
                    near = pltpu.roll(near, ((z - seg) * strip) % lon, 1)
                merged = jnp.where(group == z, near, merged) if z else near
            spent = None
            for z in range(zn + 1):
                seen = omg[seg, z, rows, :] if z < zn else merged
                resid = jnp.where(seen < 0.5 * UNSEEN, thickness(1, z, m + PAD) - seen, 0.0)
                forcing = weights[z] * resid
                part = forcing * resid
                target = cells(1, now, z, m + PAD)[0]
                keep_at(1, now, 0, z, m, target.centre() + forcing)
                if z == zn:
                    acc[0, 1, rows, :] = acc[0, 1, rows, :] + part
                else:
                    spent = part if spent is None else spent + part
            acc[0, 0, rows, :] = acc[0, 0, rows, :] + spent

        over(remaining, force)
        for n in reversed(range(SEG)):
            remaining -= 1
            later = 1 - now

            def back(m):
                rows = pl.ds(m, TILE)
                dt_drag = dragb[rows, :] * time_step
                pull = None
                for z in range(zn + 1):
                    new, part = adjoint(n, now, z, m + PAD, dt_drag)
                    for f, value in enumerate(new):
                        keep_at(1, later, f, z, m, value)
                    if z == zn:
                        acc[1, 1, rows, :] = acc[1, 1, rows, :] + part
                    else:
                        pull = part if pull is None else pull + part
                acc[1, 0, rows, :] = acc[1, 0, rows, :] + pull

            over(remaining, back)
            if n and seg:
                pass_ck(seg - 1)
            now = later

    seam_first = jnp.where(c == 0, inner // 2, reach)
    seam_end = jnp.where(c == 0, inner, reach + inner // 2)
    seam_owned = jnp.logical_and(spot >= seam_first, spot < seam_end)
    main_first = jnp.where(c == 0, 0, seam_start + seam_end)
    main_end = jnp.where(c == 0, seam_start + seam_first, 2 * lon)
    main_owned = jnp.logical_and(col >= main_first, col < main_end)
    ready = pl.ds(pl.multiple_of(base + PAD, TILE), TILE)
    for f in range(3):
        edge = lamt[now, f, ready, :]
        for z in range(zn):
            moved = pltpu.roll(edge, lax.rem(seam_start + lon - z * strip, lon), 1)
            fsend[z, f] = jnp.where(main_owned, lam[now, f, z + 1, ready, :], moved)
    scale = 1.0 / (total_lat * total_lon)
    held_rows = pl.ds(pl.multiple_of(base, TILE), TILE)
    sums = []
    for k, factor in enumerate((0.5 * scale, -time_step * scale)):
        whole = jnp.where(main_owned, acc[k, 0, held_rows, :], 0.0) + jnp.where(
            seam_owned, acc[k, 1, held_rows, :], 0.0
        )
        sums.append(factor * jnp.sum(whole, axis=1, keepdims=True))
    both = jnp.where(
        lane < lon // 2, jnp.broadcast_to(sums[0], (TILE, lon)), jnp.broadcast_to(sums[1], (TILE, lon))
    )
    for z in range(zn):
        fsend[z, 3] = both

    home = x // blocks
    slot = lax.rem(x, blocks) * 2 + g
    for dz in (2, 1, 3, 0):
        j = around(dz)
        when = None if dz else home != g
        put(fsend.at[j], frecv.at[slot], rfin.at[slot], {"gx": j, "gz": home}, when)
        put(fsend.at[j, 3], xrecv.at[slot], rxfin.at[slot], {"gx": j, "col": oc, "gz": home})

    @pl.when(home == g)
    def _():
        frecv[slot] = fsend[x]

    line = jnp.zeros((TILE, lon), f32)
    place = lax.broadcasted_iota(jnp.int32, (TILE, lon), 0) // lat
    for k in range(2 * blocks):
        j, core = g * blocks + k // 2, k % 2
        here = jnp.logical_and(x == j, g == core)
        arrived(frecv.at[k], rfin.at[k], jnp.logical_not(here))
        arrived(xrecv.at[k], rxfin.at[k])
        for f in range(3):
            out[f, k * TILE : (k + 1) * TILE, :] = frecv[k, f]
        pick = lane % (lon // 2) == k * (TILE // lat) + place
        line = line + jnp.where(pick, frecv[k, 3] + xrecv[k], 0.0)
    line = jnp.broadcast_to(jnp.sum(line, axis=0, keepdims=True), (TILE, lon))
    cost[...] = line[:1, :levels]
    dgrad[...] = pltpu.roll(line, lon // 2, 1)[:1, :levels]
    for copy, when in sent:
        if when is None:
            copy.wait_send()
        else:
            pl.when(when)(copy.wait_send)


def gathered(zn, checkpoints, obs_values, obs_mask, drag):
    segments, levels, lat, lon = obs_values.shape
    half = levels * lat
    total = 2 * half
    local_segs = checkpoints.shape[0]
    blocks = zn // 2
    sends = local_segs * blocks * (2 * zn - 1) + segments * blocks * (zn - 1)
    sends += blocks * (2 * zn - 1) + 2 * segments * blocks + blocks + 1 + 2 * zn
    f32 = jnp.float32
    dma = pltpu.SemaphoreType.DMA
    out, cost, pull = pl.pallas_call(
        functools.partial(sweep_kernel, zn, levels, lat, lon),
        out_shape=(
            jax.ShapeDtypeStruct((3, half, lon), f32),
            jax.ShapeDtypeStruct((1, levels), f32),
            jax.ShapeDtypeStruct((1, levels), f32),
        ),
        in_specs=[pl.BlockSpec(memory_space=pltpu.VMEM)] * 4,
        out_specs=[pl.BlockSpec(memory_space=pltpu.VMEM)] * 3,
        scratch_shapes=[
            pltpu.VMEM((local_segs, 2, 4, half, lon), checkpoints.dtype),
            pltpu.VMEM((2, half, lon), f32),
            pltpu.VMEM((segments, 4, zn, total, lon), checkpoints.dtype),
            pltpu.VMEM((segments, zn, total, lon), f32),
            pltpu.VMEM((2, zn, total, lon), f32),
            pltpu.VMEM((total, lon), f32),
            pltpu.VMEM((2, 3, zn + 2, total + 2 * PAD, lon), f32),
            pltpu.VMEM((2, 3, total + 2 * PAD, lon), f32),
            pltpu.VMEM((2, 3, zn + 2, total + 2 * PAD, lon), f32),
            pltpu.VMEM((2, 3, total + 2 * PAD, lon), f32),
            pltpu.VMEM((2, 2, total, lon), f32),
            pltpu.VMEM((zn, 4, TILE, lon), f32),
            pltpu.VMEM((2 * blocks, 4, TILE, lon), f32),
            pltpu.VMEM((2 * blocks, TILE, lon), f32),
            dma((sends,)),
            dma((segments, zn, blocks)),
            dma((segments, blocks)),
            dma((segments, zn, blocks)),
            dma((segments, blocks)),
            dma((2, zn, blocks)),
            dma((blocks,)),
            dma,
            dma((2 * blocks,)),
            dma((2 * blocks,)),
        ],
        compiler_params=pltpu.CompilerParams(
            collective_id=0, has_side_effects=True, vmem_limit_bytes=48 * 2**20
        ),
        name="sweep",
    )(
        checkpoints.reshape(local_segs, 3, half, 2 * lon),
        obs_values.reshape(segments, half, lon),
        obs_mask.reshape(segments, half, lon),
        drag.reshape(1, levels),
    )
    return out.reshape(3, levels, lat, lon), cost.reshape(levels), pull.reshape(levels)


def choose(sizes, checkpoints, obs_values, obs_mask, drag):
    segments, levels, lat, lon = obs_values.shape
    zn = sizes["gx"]
    total = 2 * levels * lat
    reach = SEG * (segments + 1)
    fits = (
        sizes["col"] == 2
        and sizes["gz"] == 2
        and zn == 4
        and segments == 2 * checkpoints.shape[0] == 4
        and TILE % lat == 0
        and total == 2 * zn * TILE
        and lon == 128
        and lon // zn >= 3 * reach + 2
        and reach * lat <= 3 * TILE
        and (reach - SEG) * lat <= 2 * TILE
        and levels <= lon // 2
    )
    if fits:
        return gathered(zn, checkpoints, obs_values, obs_mask, drag)
    return on_device(checkpoints, obs_values, obs_mask, drag)


def solution(mesh):
    sizes = dict(mesh.shape)
    return jax.shard_map(
        functools.partial(choose, sizes),
        mesh=mesh,
        in_specs=(
            P(("ens", "col"), None, "gz", "gx", None),
            P("ens", "gz", "gx", "col"),
            P("ens", "gz", "gx", "col"),
            P(("ens", "gz")),
        ),
        out_specs=(P("ens", "gz", "gx", "col"), P(("ens", "gz")), P(("ens", "gz"))),
        check_vma=False,
    )
```
